512 devices in a mesh: ep: 128 (over x, z, core), dp: 4 (over y).
Axes of the slice: x: 4, y: 4, z: 16, core: 2. Of those that a mesh axis runs over, the one named last changes fastest.
Arguments:
- tokens: bfloat16 [2048, 3584], P('ep'), may hold values from -6 to 6
- expert_ids: int32 [2048, 8], P('ep'), may hold values from 0 to 127, all different within a row; in each aligned block of 16 rows (0 to 15, 16 to 31, ...) at most 4 rows name the same one
- route_logits: float32 [2048, 8], P('ep'), may hold values from -8 to 8
- expert_gate: bfloat16 [128, 3584, 1024], P('ep', None, 'dp'), may hold values from -0.09375 to 0.09375
- expert_up: bfloat16 [128, 3584, 1024], P('ep', None, 'dp'), may hold values from -0.09375 to 0.09375
- expert_down: bfloat16 [128, 1024, 3584], P('ep', 'dp'), may hold values from -0.1875 to 0.1875
Outputs:
- mixed: bfloat16 [2048, 3584], P(('ep', 'dp'))
The draws below stay inside these ranges and needn't reach their ends.
Inputs may be any that keep to these rules, and one draw needn't show every extreme that they name: `expert_ids`: each row names 8 different experts of 0 to 127 and every expert is named by some row. Within the rows of one index of ep (aligned blocks of 16 rows) no expert is named more than 4 times, and some block names one expert exactly 4 times. Loads are heavy-tailed: a few experts take several times the mean.
All inputs are finite; a program needn't handle non-finite values.
Results may differ from the reference program's by a relative error of at most 0.015.
Values may be sent and summed in bfloat16 or wider, within the bound.
A program may use at most 64 MiB of HBM per device.

```python
import math
import jax
import jax.numpy as jnp
import numpy as np
from jax import lax

D = 3584
FF = 1024
TOP = 8
TOK_EP = 16
EXPERTS = 128
TOKENS = 2048
CAP = 4


def block_levels(own_key, shape, cuts, smallest, largest):
    gain = 1.0
    for position, parts in cuts:
        steps = jax.random.uniform(jax.random.fold_in(jax.random.fold_in(own_key, 6), position), (parts,), jnp.float32, smallest / len(cuts), largest / len(cuts))
        gain = gain * jnp.repeat(jnp.exp(steps), shape[position] // parts).reshape((-1,) + (1,) * (len(shape) - 1 - position))
    return gain


def deal_out(key, own, number, rows, amount, top, reach, lean):
    sequence = jax.random.permutation(key, amount)
    heavy_load, usual = load_shares(amount, rows * top, reach, lean, True), load_shares(amount, rows * top, reach, lean, False)
    places = jnp.arange(amount)

    def named(tallies, rotation):
        used = int((tallies > 0).sum())
        fixed = max(1, used // 4)
        shifted = fixed + (places - fixed + rotation * (used - fixed)) % max(1, amount - fixed)
        return jnp.zeros((amount,), jnp.int32).at[sequence[jnp.where(places < fixed, places, shifted)]].set(jnp.asarray(tallies, jnp.int32))

    tallies = jnp.where(number % 4 == 0, named(heavy_load, number // 4), named(usual, number - number // 4 - 1))
    mixed = jax.random.permutation(jax.random.fold_in(own, 3), amount)
    donor, taker = mixed[0:amount // 2 * 2:2], mixed[1:amount // 2 * 2:2]
    margin = jnp.minimum(tallies[donor] - 1, reach - tallies[taker]) // 2
    margin = jnp.where((donor == sequence[0]) | (taker == sequence[0]) | (tallies[taker] == 0), 0, jnp.maximum(margin, 0))
    shifted = jax.random.randint(jax.random.fold_in(own, 4), (amount // 2,), 0, 1 << 20) % (margin + 1)
    tallies = tallies.at[donor].add(-shifted).at[taker].add(shifted)
    members = jnp.searchsorted(jnp.cumsum(tallies), jnp.arange(rows * top), side="right").astype(jnp.int32)
    listing = members.reshape(top, rows).T
    listing = listing[jax.random.permutation(jax.random.fold_in(own, 1), rows)]
    rotation = jax.random.randint(jax.random.fold_in(own, 2), (rows, 1), 0, top)
    return jnp.take_along_axis(listing, (jnp.arange(top)[None, :] + rotation) % top, axis=1)


def load_shares(count, total, bound, slope, full):
    loads = [(1 << 20) // math.isqrt(standing ** slope) + 1 for standing in range(1, count + 1)]
    largest = bound if full else min(bound, max(-(-total // count), total * loads[0] // sum(loads)))
    least = 1 if total - largest >= count - 1 else 0
    given, spare = [largest] + [least] * (count - 1), total - largest - least * (count - 1)
    while spare > 0:
        free = [i for i in range(1, count) if given[i] < largest] or [i for i in range(1, count) if given[i] < bound]
        pool, remaining = sum([loads[i] for i in free]), spare
        for i in free:
            extra = min(bound - given[i], max(1, remaining * loads[i] // pool), spare)
            given[i] = given[i] + extra
            spare = spare - extra
    return np.array(given)


def scatter_about(rng, extent, scale, most, cuts=(), held_as=jnp.bfloat16):
    result = jax.random.normal(rng, extent, jnp.float32) * scale
    if len(cuts) > 0:
        result = block_levels(rng, extent, cuts, -0.22, 0.18) * result
    return jnp.clip(result, min=-most, max=most).astype(held_as)


def setup_inputs(seed: int = 0) -> dict:
    key_of = jax.random.split(jax.random.key(seed), 7)
    tokens = scatter_about(key_of[0], (TOKENS, D), 1.0, 6.0, ((0, 128),))
    expert_ids_keys = jax.random.split(jax.random.fold_in(key_of[1], 1), TOKENS // TOK_EP)
    expert_ids_turns = jax.random.permutation(jax.random.fold_in(key_of[1], 3), TOKENS // TOK_EP)
    expert_ids = jax.vmap(lambda own, number: deal_out(jax.random.fold_in(key_of[1], 2), own, number, TOK_EP, EXPERTS, TOP, CAP, 3))(expert_ids_keys, expert_ids_turns).reshape((TOKENS, TOP))
    route_logits = scatter_about(key_of[2], (TOKENS, TOP), 2.0, 8.0, ((0, 128),), jnp.float32)
    expert_gate = scatter_about(key_of[3], (EXPERTS, D, FF), D ** -0.5, 0.09375, ((0, 128), (2, 4)))
    expert_up = scatter_about(key_of[4], (EXPERTS, D, FF), D ** -0.5, 0.09375, ((0, 128), (2, 4)))
    expert_down = scatter_about(key_of[5], (EXPERTS, FF, D), FF ** -0.5, 0.1875, ((0, 128), (1, 4)))
    return dict(tokens=tokens, expert_ids=expert_ids, route_logits=route_logits, expert_gate=expert_gate, expert_up=expert_up, expert_down=expert_down)


route_scale = 2.5


def expert_rows(rows, w_gate, w_up, w_down):
    gate = jnp.dot(rows, w_gate, preferred_element_type=jnp.float32)
    upper = jnp.dot(rows, w_up, preferred_element_type=jnp.float32)
    hidden = (jax.nn.silu(gate) * upper).astype(jnp.bfloat16)
    return jnp.dot(hidden, w_down, preferred_element_type=jnp.float32).astype(jnp.bfloat16)


def reference(tokens, expert_ids, route_logits, expert_gate, expert_up, expert_down):
    token_count, width = tokens.shape
    top = expert_ids.shape[1]
    experts = expert_gate.shape[0]
    flat_ids = expert_ids.reshape(-1).astype(jnp.int32)
    slots = flat_ids.shape[0]
    block_rows = 64
    counts = jnp.zeros((experts,), jnp.int32).at[flat_ids].add(1).astype(jnp.int32)
    padded = (((counts + block_rows - 1) // block_rows) * block_rows).astype(jnp.int32)
    pad_start = (jnp.cumsum(padded) - padded).astype(jnp.int32)
    seg_start = (jnp.cumsum(counts) - counts).astype(jnp.int32)
    sorted_slots = jnp.argsort(flat_ids, stable=True).astype(jnp.int32)
    sorted_ids = flat_ids[sorted_slots]
    within = (jnp.arange(slots, dtype=jnp.int32) - seg_start[sorted_ids]).astype(jnp.int32)
    target = (pad_start[sorted_ids] + within).astype(jnp.int32)
    nblocks = (slots + experts * (block_rows - 1)) // block_rows + 1
    row_token = jnp.full((nblocks * block_rows,), token_count, jnp.int32).at[target].set((sorted_slots // top).astype(jnp.int32))
    pad_end = pad_start + padded
    block_start = jnp.arange(nblocks, dtype=jnp.int32) * block_rows
    block_expert = jnp.sum((pad_end[None, :] <= block_start[:, None]).astype(jnp.int32), axis=1)
    block_expert = jnp.minimum(block_expert, experts - 1).astype(jnp.int32)
    extended = jnp.concatenate([tokens, jnp.zeros((1, width), tokens.dtype)], axis=0)

    def one_block(inputs):
        block_index, expert = inputs
        picks = lax.dynamic_slice_in_dim(row_token, (block_index * block_rows).astype(jnp.int32), block_rows, 0)
        return expert_rows(extended[picks], expert_gate[expert], expert_up[expert], expert_down[expert])

    outputs = lax.map(one_block, (jnp.arange(nblocks, dtype=jnp.int32), block_expert))
    outputs = outputs.reshape(nblocks * block_rows, width)
    slot_target = jnp.zeros((slots,), jnp.int32).at[sorted_slots].set(target)
    slot_values = outputs[slot_target].reshape(token_count, top, width)
    scores = jax.nn.sigmoid(route_logits)
    weights = route_scale * scores / jnp.sum(scores, axis=1, keepdims=True)
    routed = jnp.sum(weights[:, :, None] * slot_values.astype(jnp.float32), axis=1)
    return routed.astype(jnp.bfloat16)
```

```python
import functools

import jax
import jax.numpy as jnp
from jax import lax
from jax.experimental import pallas as pl
from jax.experimental.pallas import tpu as pltpu
from jax.sharding import PartitionSpec as P

route_scale = 2.5
MESH = pl.DeviceIdType.MESH
NX = 4
NZ = 16
ROWS = 16
HALF = NZ // 2
NEAR = HALF - 1
LANES = 128
ZA_GATHER = 11 * LANES
ZA_SCATTER = 10 * LANES
f32 = jnp.float32
bf16 = jnp.bfloat16


def place():
    ep = lax.axis_index("ep")
    y = lax.axis_index("dp")
    core = lax.rem(ep, 2)
    z = lax.rem(ep // 2, NZ)
    x = ep // (2 * NZ)

    def dev(x_, z_, core_):
        return ((lax.rem(x_ + NX, NX) * NZ + lax.rem(z_ + NZ, NZ)) * 2 + core_, y)

    return ep, x, y, z, core, dev


def remote(src, dst, send, recv, device):
    return pltpu.make_async_remote_copy(
        src_ref=src, dst_ref=dst, send_sem=send, recv_sem=recv, device_id=device, device_id_type=MESH
    )


def greet(peers):
    barrier = pltpu.get_barrier_semaphore()
    for device in peers:
        pl.semaphore_signal(barrier, inc=1, device_id=device, device_id_type=MESH)
    return barrier


def within(k, low, high):
    return jnp.logical_and(k >= low, k <= high)


def gather_kernel(
    tok, ids, logits, wg_hbm, wu_hbm, hid,
    ga, gb, wg, wu, wsem, ax_s, ax_r, za_s, za_r, zb_s, zb_r, xb_s, xb_r, ca_s, ca_r, cb_s, cb_r,
):
    ep, x, y, z, core, dev = place()
    fa = ga.shape[-1]
    fb = gb.shape[-1] - LANES
    other = 1 - core
    barrier = greet(
        [dev(x + 1, z, core), dev(x + 3, z, core), dev(x + 2, z, core), dev(x, z + 1, core), dev(x, z + 15, core), dev(x, z, other)]
    )
    copy_g = pltpu.make_async_copy(wg_hbm.at[0], wg, wsem.at[0])
    copy_u = pltpu.make_async_copy(wu_hbm.at[0], wu, wsem.at[1])
    copy_g.start()
    copy_u.start()

    ga[z, 0, x] = tok[:, :fa]
    gb[z, 0, x, :, :fb] = tok[:, fa:]
    scores = jax.nn.sigmoid(logits[...])
    weights = route_scale * scores / jnp.sum(scores, axis=1, keepdims=True)
    names = ids[...]
    lane = lax.broadcasted_iota(jnp.int32, (ROWS, LANES), 1)
    table = jnp.zeros((ROWS, LANES), f32)
    for k in range(8):
        table = table + jnp.where(names[:, k : k + 1] == lane, weights[:, k : k + 1], 0.0)
    gb[z, 0, x, :, fb:] = table.astype(bf16)
    pl.semaphore_wait(barrier, 6)

    def zdev(s):
        return dev(x, z + 1, core) if s == 0 else dev(x, z + 15, core)

    def at(s, k):
        return lax.rem(z + NZ - k, NZ) if s == 0 else lax.rem(z + k, NZ)

    def ax(j):
        return remote(ga.at[z, 0, x], ga.at[z, 0, x], ax_s.at[j], ax_r.at[j], dev(x + j + 1, z, core))

    def za(s, h, k, d):
        ref = ga.at[d, 0, pl.ds(2 * h, 2)]
        return remote(ref, ref, za_s.at[s, h, k], za_r.at[s, h, k], zdev(s))

    def zb(s, k, d):
        ref = gb.at[d, 0, x]
        return remote(ref, ref, zb_s.at[s, k], zb_r.at[s, k], zdev(s))

    def xb(d, j, row, step):
        ref = gb.at[d, 0, lax.rem(row + NX, NX)]
        return remote(ref, ref, xb_s.at[d, j], xb_r.at[d, j], dev(x + step, z, core))

    def ca(d):
        return remote(ga.at[d, 0], ga.at[d, 1], ca_s.at[d], ca_r.at[d], dev(x, z, other))

    def cb(d):
        return remote(gb.at[d, 0], gb.at[d, 1], cb_s.at[d], cb_r.at[d], dev(x, z, other))

    for j in range(3):
        ax(j).start()
    for s in range(2):
        zb(s, 1, z).start()
    xb(z, 0, x, 1).start()
    xb(z, 1, x, 3).start()
    for j in range(3):
        ax(j).wait_recv()
    for h in range(2):
        for s in range(2):
            za(s, h, 1, z).start()
    copy_g.wait()
    copy_u.wait()

    def mine(s, k):
        return within(k, 0, NEAR) if s == 0 else within(k, 1, HALF)

    def compute(d):
        ca(d).wait_recv()
        cb(d).wait_recv()
        rows_a = ga[d].reshape(2 * NX * ROWS, fa)
        rows_b = gb[d, :, :, :, :fb].reshape(2 * NX * ROWS, fb)
        side = gb[d, :, :, :, fb:].reshape(2 * NX * ROWS, LANES).astype(f32)
        here = lax.broadcasted_iota(jnp.int32, side.shape, 1) == ep
        scale = jnp.sum(jnp.where(here, side, 0.0), axis=1, keepdims=True)
        gate = jnp.dot(rows_a, wg[:fa, :], preferred_element_type=f32) + jnp.dot(rows_b, wg[fa:, :], preferred_element_type=f32)
        upper = jnp.dot(rows_a, wu[:fa, :], preferred_element_type=f32) + jnp.dot(rows_b, wu[fa:, :], preferred_element_type=f32)
        hidden = gate / (1.0 + jnp.exp(-gate)) * upper * scale
        hid[d] = hidden.astype(bf16).reshape(2, NX, ROWS, hidden.shape[-1])

    def step(k, carry):
        for s in range(2):
            top = NEAR if s == 0 else HALF

            @pl.when(within(k, 1, top))
            def _():
                d = at(s, k)
                zb(s, k, d).wait_recv()

                @pl.when(k < top)
                def _():
                    zb(s, k + 1, d).start()

                xb(d, 0, x, 1).start()
                xb(d, 1, x, 3).start()

        for h in range(2):
            for s in range(2):
                top = HALF if s == h else NEAR

                @pl.when(within(k, 1, top))
                def _():
                    d = at(s, k)
                    za(s, h, k, d).wait_recv()

                    @pl.when(k < top)
                    def _():
                        za(s, h, k + 1, d).start()

        for s in range(2):

            @pl.when(mine(s, k))
            def _():
                ca(at(s, k)).start()

        for s in range(2):

            @pl.when(mine(s, k - 1))
            def _():
                d = at(s, k - 1)
                xb(d, 0, x + 3, 1).wait_recv()
                xb(d, 1, x + 1, 1).wait_recv()
                if s == 0:
                    xb(d, 2, x + 3, 1).start()
                else:
                    xb(d, 2, x + 1, 3).start()

        for s in range(2):

            @pl.when(mine(s, k - 2))
            def _():
                d = at(s, k - 2)
                xb(d, 2, x + 2, 1).wait_recv()
                cb(d).start()

        for s in range(2):

            @pl.when(mine(s, k - 3))
            def _():
                compute(at(s, k - 3))

        return carry

    lax.fori_loop(0, HALF + 4, step, 0)

    for j in range(3):
        ax(j).wait_send()

    def drain(k, carry):
        for s in range(2):
            top = NEAR if s == 0 else HALF

            @pl.when(k <= top)
            def _():
                zb(s, k, z).wait_send()

        for h in range(2):
            for s in range(2):
                top = HALF if s == h else NEAR

                @pl.when(k <= top)
                def _():
                    za(s, h, k, z).wait_send()

        return carry

    lax.fori_loop(1, HALF + 1, drain, 0)

    def drain_all(d, carry):
        for j in range(3):
            xb(d, j, x, 1).wait_send()
        ca(d).wait_send()
        cb(d).wait_send()
        return carry

    lax.fori_loop(0, NZ, drain_all, 0)


def scatter_kernel(
    hid, wd_hbm, out,
    wd, own, sib_out, sib_in, a_out, a_in, b_out, b_in, x_out, x_in, f_out, f_in, y_out, y_in,
    wsem, c_s, c_r, a_s, a_r, b_s, b_r, x_s, x_r, f_s, f_r, y_s, y_r,
):
    ep, x, y, z, core, dev = place()
    width = own.shape[-1]
    fa = a_out.shape[-1]
    fb = width - fa
    other = 1 - core
    n_dp = y_out.shape[0]

    def ydev(j):
        return (ep, lax.rem(y + j, n_dp))

    barrier = greet(
        [dev(x + 1, z, core), dev(x + 3, z, core), dev(x + 2, z, core), dev(x, z + 1, core), dev(x, z + 15, core), dev(x, z, other)]
        + [ydev(j) for j in range(1, n_dp)]
    )
    copy_d = pltpu.make_async_copy(wd_hbm.at[0], wd, wsem)
    copy_d.start()
    pl.semaphore_wait(barrier, 6 + n_dp - 1)
    copy_d.wait()

    def at(s, k):
        return lax.rem(z + k, NZ) if s == 0 else lax.rem(z + NZ - k, NZ)

    def zdev(s):
        return dev(x, z + 1, core) if s == 0 else dev(x, z + 15, core)

    def xmod(v):
        return lax.rem(v + NX, NX)

    def cc(d):
        return remote(sib_out.at[d], sib_in.at[d], c_s.at[d], c_r.at[d], dev(x, z, other))

    def ra(s, h, k):
        return remote(a_out.at[s, h, k], a_in.at[s, h, k], a_s.at[s, h, k], a_r.at[s, h, k], zdev(s))

    def rb(s, k):
        return remote(b_out.at[s, k], b_in.at[s, k], b_s.at[s, k], b_r.at[s, k], zdev(s))

    def rx(d, j, step):
        return remote(x_out.at[d, j], x_in.at[d, j], x_s.at[d, j], x_r.at[d, j], dev(x + step, z, core))

    def rf(j):
        return remote(f_out.at[j], f_in.at[j], f_s.at[j], f_r.at[j], dev(x + j + 1, z, core))

    def ry(j):
        return remote(y_out.at[lax.rem(y + j, n_dp)], y_in.at[j], y_s.at[j], y_r.at[j], ydev(j))

    def term_a(d, h):
        rows = pl.ds(2 * h, 2)
        return own[d, rows, :, :fa].astype(f32) + sib_in[d, rows, :, :fa].astype(f32)

    def term_b(d, row):
        return own[d, row, :, fa:].astype(f32) + sib_in[d, row, :, fa:].astype(f32)

    def project(d):
        rows = hid[d].reshape(2 * NX * ROWS, hid.shape[-1])
        cut = 512

        def piece(n, carry):
            columns = pl.ds(pl.multiple_of(n * cut, cut), cut)
            value = jnp.dot(rows, wd[:, columns], preferred_element_type=f32).astype(bf16)
            value = value.reshape(2, NX, ROWS, cut)
            own[d, :, :, columns] = value[0]
            sib_out[d, :, :, columns] = value[1]
            return carry

        lax.fori_loop(0, width // cut, piece, 0)
        cc(d).start()

    def has(s, k):
        return within(k, 0, NEAR) if s == 0 else within(k, 1, HALF)

    def step(t, carry):
        k0 = HALF - t
        for s in range(2):

            @pl.when(has(s, k0))
            def _():
                project(at(s, k0))

        k1 = HALF + 1 - t
        for s in range(2):

            @pl.when(has(s, k1))
            def _():
                cc(at(s, k1)).wait_recv()

        for h in range(2):
            for s in range(2):
                top = HALF if s == h else NEAR

                @pl.when(k1 == top)
                def _():
                    d = at(s, k1)
                    a_out[s, h, k1] = term_a(d, h).astype(bf16)
                    ra(s, h, k1).start()

                @pl.when(within(k1, 1, top - 1))
                def _():
                    d = at(s, k1)
                    ra(s, h, k1 + 1).wait_recv()
                    a_out[s, h, k1] = (term_a(d, h) + a_in[s, h, k1 + 1].astype(f32)).astype(bf16)
                    ra(s, h, k1).start()

        for s in range(2):
            go, back = (1, 3) if s == 0 else (3, 1)

            @pl.when(has(s, k1))
            def _():
                d = at(s, k1)
                x_out[d, 0] = term_b(d, xmod(x + 2)).astype(bf16)
                rx(d, 0, go).start()
                x_out[d, 1] = term_b(d, xmod(x + back)).astype(bf16)
                rx(d, 1, back).start()

        k2 = HALF + 2 - t
        for s in range(2):
            go, back = (1, 3) if s == 0 else (3, 1)

            @pl.when(has(s, k2))
            def _():
                d = at(s, k2)
                rx(d, 0, go).wait_recv()
                x_out[d, 2] = (term_b(d, xmod(x + go)) + x_in[d, 0].astype(f32)).astype(bf16)
                rx(d, 2, go).start()

        k3 = HALF + 3 - t
        for s in range(2):
            top = NEAR if s == 0 else HALF

            @pl.when(jnp.logical_and(has(s, k3), k3 >= 1))
            def _():
                d = at(s, k3)
                rx(d, 1, 1).wait_recv()
                rx(d, 2, 1).wait_recv()
                total = term_b(d, x) + x_in[d, 1].astype(f32) + x_in[d, 2].astype(f32)

                @pl.when(k3 == top)
                def _():
                    b_out[s, k3] = total.astype(bf16)

                @pl.when(k3 < top)
                def _():
                    rb(s, k3 + 1).wait_recv()
                    b_out[s, k3] = (total + b_in[s, k3 + 1].astype(f32)).astype(bf16)

                rb(s, k3).start()

        return carry

    lax.fori_loop(0, HALF + 3, step, 0)

    for h in range(2):
        for s in range(2):
            ra(s, h, 1).wait_recv()
    for j in range(3):
        row = xmod(x + j + 1)
        sums = own[z, row, :, :fa].astype(f32) + sib_in[z, row, :, :fa].astype(f32)
        sums = sums + a_in[0, row // 2, 1, lax.rem(row, 2)].astype(f32) + a_in[1, row // 2, 1, lax.rem(row, 2)].astype(f32)
        f_out[j] = sums.astype(bf16)
        rf(j).start()
    total_a = own[z, x, :, :fa].astype(f32) + sib_in[z, x, :, :fa].astype(f32)
    total_a = total_a + a_in[0, x // 2, 1, lax.rem(x, 2)].astype(f32) + a_in[1, x // 2, 1, lax.rem(x, 2)].astype(f32)

    rx(z, 1, 1).wait_recv()
    rx(z, 2, 1).wait_recv()
    total_b = term_b(z, x) + x_in[z, 1].astype(f32) + x_in[z, 2].astype(f32)
    for s in range(2):
        rb(s, 1).wait_recv()
        total_b = total_b + b_in[s, 1].astype(f32)
    for j in range(3):
        rf(j).wait_recv()
        total_a = total_a + f_in[j].astype(f32)
    part = ROWS // n_dp
    for j in range(n_dp):
        y_out[j, :, :fa] = total_a[part * j : part * (j + 1)]
        y_out[j, :, fa:] = total_b[part * j : part * (j + 1)]
    for j in range(1, n_dp):
        ry(j).start()
    result = y_out[y]
    for j in range(1, n_dp):
        ry(j).wait_recv()
        result = result + y_in[j]
    out[...] = result.astype(bf16)

    for j in range(1, n_dp):
        ry(j).wait_send()
    for j in range(3):
        rf(j).wait_send()

    def drain(k, carry):
        for s in range(2):
            top = NEAR if s == 0 else HALF

            @pl.when(k <= top)
            def _():
                rb(s, k).wait_send()

        for h in range(2):
            for s in range(2):
                top = HALF if s == h else NEAR

                @pl.when(k <= top)
                def _():
                    ra(s, h, k).wait_send()

        return carry

    lax.fori_loop(1, HALF + 1, drain, 0)

    def drain_all(d, carry):
        for j in range(3):
            rx(d, j, 1).wait_send()
        cc(d).wait_send()
        return carry

    lax.fori_loop(0, NZ, drain_all, 0)


def on_device(tokens, expert_ids, route_logits, expert_gate, expert_up, expert_down):
    width = tokens.shape[1]
    n_dp = lax.axis_size("dp")
    cut = expert_gate.shape[2]
    vmem = pl.BlockSpec(memory_space=pltpu.VMEM)
    whole = pl.BlockSpec(memory_space=pl.ANY)
    dma = pltpu.SemaphoreType.DMA
    fa, fb = ZA_GATHER, width - ZA_GATHER
    hidden = pl.pallas_call(
        gather_kernel,
        name="gather_up",
        out_shape=jax.ShapeDtypeStruct((NZ, 2, NX, ROWS, cut), bf16),
        in_specs=[vmem, vmem, vmem, whole, whole],
        out_specs=vmem,
        scratch_shapes=[
            pltpu.VMEM((NZ, 2, NX, ROWS, fa), bf16),
            pltpu.VMEM((NZ, 2, NX, ROWS, fb + LANES), bf16),
            pltpu.VMEM((width, cut), bf16),
            pltpu.VMEM((width, cut), bf16),
            dma((2,)),
            dma((3,)), dma((3,)),
            dma((2, 2, HALF + 1)), dma((2, 2, HALF + 1)),
            dma((2, HALF + 1)), dma((2, HALF + 1)),
            dma((NZ, 3)), dma((NZ, 3)),
            dma((NZ,)), dma((NZ,)),
            dma((NZ,)), dma((NZ,)),
        ],
        compiler_params=pltpu.CompilerParams(collective_id=0, has_side_effects=True, vmem_limit_bytes=48 * 2**20),
    )(tokens, expert_ids, route_logits, expert_gate, expert_up)
    fa = ZA_SCATTER
    fb = width - fa
    part = ROWS // n_dp
    return pl.pallas_call(
        scatter_kernel,
        name="down_scatter",
        out_shape=jax.ShapeDtypeStruct((part, width), bf16),
        in_specs=[vmem, whole],
        out_specs=vmem,
        scratch_shapes=[
            pltpu.VMEM((cut, width), bf16),
            pltpu.VMEM((NZ, NX, ROWS, width), bf16),
            pltpu.VMEM((NZ, NX, ROWS, width), bf16),
            pltpu.VMEM((NZ, NX, ROWS, width), bf16),
            pltpu.VMEM((2, 2, HALF + 1, 2, ROWS, fa), bf16),
            pltpu.VMEM((2, 2, HALF + 1, 2, ROWS, fa), bf16),
            pltpu.VMEM((2, HALF + 1, ROWS, fb), bf16),
            pltpu.VMEM((2, HALF + 1, ROWS, fb), bf16),
            pltpu.VMEM((NZ, 3, ROWS, fb), bf16),
            pltpu.VMEM((NZ, 3, ROWS, fb), bf16),
            pltpu.VMEM((3, ROWS, fa), bf16),
            pltpu.VMEM((3, ROWS, fa), bf16),
            pltpu.VMEM((n_dp, part, width), f32),
            pltpu.VMEM((n_dp, part, width), f32),
            dma,
            dma((NZ,)), dma((NZ,)),
            dma((2, 2, HALF + 1)), dma((2, 2, HALF + 1)),
            dma((2, HALF + 1)), dma((2, HALF + 1)),
            dma((NZ, 3)), dma((NZ, 3)),
            dma((3,)), dma((3,)),
            dma((n_dp,)), dma((n_dp,)),
        ],
        compiler_params=pltpu.CompilerParams(collective_id=1, has_side_effects=True, vmem_limit_bytes=60 * 2**20),
    )(hidden, expert_down)


def solution(mesh):
    placed = (
        P("ep", None),
        P("ep", None),
        P("ep", None),
        P("ep", None, "dp"),
        P("ep", None, "dp"),
        P("ep", "dp", None),
    )
    return jax.shard_map(
        on_device, mesh=mesh, in_specs=placed, out_specs=P(("ep", "dp"), None), check_vma=False
    )
```
